32 devices in a mesh: ma: 8 (over z, x), lev: 4 (over y, core).
Axes of the slice: x: 2, y: 2, z: 4, core: 2. Of those that a mesh axis runs over, the one named last changes fastest.
Arguments:
- forcing: float32 [72, 2, 1280, 1280], P('lev', None, 'ma'), may hold values from -80 to 80
- coupling: float32 [4, 1280, 1280], P(None, 'ma'), may hold values from -0.3 to 0.3
- helmholtz: float32 [1280], replicated, may hold values from 0.5 to 5
- vertical: float32 [72, 72], replicated, may hold values from -1 to 3, as said below
Outputs:
- solution: float32 [72, 2, 1280, 1280], P('lev', None, 'ma')
- norms: float32 [2], replicated
The draws below stay inside these ranges and needn't reach their ends.
Inputs may be any that keep to these rules, and one draw needn't show every extreme that they name: `vertical`: the diagonal entries lie between 1 and 3.
All inputs are finite; a program needn't handle non-finite values.
Results may differ from the reference program's by a relative error of at most 0.000071.
Values sent between devices are 32-bit elements; how exact they have to be, the bound alone decides.
A program may use at most 704 MiB of HBM per device.

```python
import math
import jax
import jax.numpy as jnp
from jax import lax

LEV = 72
WAVES = 1280
N_MA = 8


def draw_forcing(key, part):
    base_key, row_key, col_key = jax.random.split(jax.random.fold_in(key, 11), 3)
    shape = (LEV, 2, WAVES, WAVES)
    rows = jnp.arange(WAVES, dtype=jnp.float32)
    ramp = 1.0 + rows / WAVES
    spread = jnp.exp(jax.random.uniform(row_key, (WAVES,), jnp.float32, math.log(0.25), math.log(2.5)))
    columns = jnp.exp(jax.random.uniform(col_key, (WAVES,), jnp.float32, math.log(0.3), math.log(3.0)))
    base = jax.random.truncated_normal(base_key, -4.0, 4.0, shape, jnp.float32)
    return base * (ramp * spread)[None, None, :, None] * columns[None, None, None, :]


def draw_vertical(key, part):
    diag_key, off_key = jax.random.split(jax.random.fold_in(key, 23), 2)
    diagonal = jax.random.uniform(diag_key, (LEV,), jnp.float32, 1.0, 3.0)
    offdiag = jax.random.truncated_normal(off_key, -4.0, 4.0, (LEV, LEV), jnp.float32) / LEV
    identity = jnp.eye(LEV, dtype=jnp.float32)
    return offdiag * (1.0 - identity) + diagonal[None, :] * identity


def block_scale(own_key, shape, cuts, low, largest):
    level, own = 1.0, jax.random.fold_in(own_key, 6)
    for position, shards_of in cuts:
        steps = jnp.exp(jax.random.uniform(jax.random.fold_in(own, position), (shards_of,), jnp.float32, low / len(cuts), largest / len(cuts)))
        level = level * jnp.repeat(steps, shape[position] // shards_of).reshape([-1 if axis == position else 1 for axis in range(len(shape))])
    return level


def setup_inputs(seed: int = 0) -> dict:
    seeds = jax.random.split(jax.random.key(seed), 5)
    return {
        "forcing": draw_forcing(jax.random.fold_in(seeds[4], 71), 0),
        "coupling": jnp.clip(jax.random.uniform(seeds[1], (4, WAVES, WAVES), jnp.float32, -0.3, 0.3) * block_scale(seeds[1], (4, WAVES, WAVES), ((1, 8),), -0.4, 0.0), -0.3, 0.3),
        "helmholtz": jnp.clip(jnp.exp(jax.random.uniform(seeds[2], (WAVES,), jnp.float32, math.log(0.5), math.log(5.0))), 0.5, 5.0),
        "vertical": draw_vertical(jax.random.fold_in(seeds[4], 71), 0),
    }


OFFSETS = (-2, -1, 1, 2)

def storage_waves():
    per_owner = WAVES // N_MA
    place = jnp.arange(WAVES, dtype=jnp.int32)
    owner = place // per_owner
    fold = place % per_owner
    return fold * N_MA + jnp.where(fold % 2 == 0, owner, N_MA - 1 - owner)

def reference(forcing, coupling, helmholtz, vertical):
    waves = storage_waves()
    row_of_wave = jnp.argsort(waves).astype(jnp.int32)
    positions = jnp.arange(WAVES, dtype=jnp.int32)
    live = (positions[None, :] >= waves[:, None]).astype(jnp.float32)[None, None]
    scale = 1.0 / (1.0 + helmholtz[None, :] * jnp.diagonal(vertical)[:, None])
    scale = scale[:, None, None, :]

    def operator(values):
        mixed = jnp.einsum('kl,lcin->kcin', vertical, values, precision=lax.Precision.HIGHEST)
        result = values + helmholtz[None, None, None, :] * mixed
        for place, offset in enumerate(OFFSETS):
            target = waves + offset
            valid = ((target >= 0) & (target < WAVES)).astype(jnp.float32)
            source = row_of_wave[jnp.clip(target, 0, WAVES - 1)].astype(jnp.int32)
            moved = jnp.take(values, source, axis=2) * valid[None, None, :, None]
            result = result + coupling[place][None, None] * moved
        return result * live
    rhs = forcing * live
    first = scale * rhs
    residual = rhs - operator(first)
    solution = first + scale * residual
    count = LEV * WAVES * (WAVES + 1)
    sums = jnp.stack([jnp.sum(rhs * rhs), jnp.sum(residual * residual)])
    norms = jnp.sqrt(sums / count)
    return (solution, norms)
```

```python
import functools

import jax
import jax.numpy as jnp
from jax import lax
from jax.experimental import pallas as pl
from jax.experimental.pallas import tpu as pltpu
from jax.sharding import PartitionSpec as P

OFFSETS = (-2, -1, 1, 2)
COLUMN_STEP = 256


def shifted(block, axis, distance):
    devices = range(lax.axis_size(axis))
    route = [(i - distance, i) for i in devices if i - distance in devices]
    return lax.ppermute(block, axis, route)


def swapped(block, axis):
    return lax.ppermute(block, axis, [(i, i ^ 1) for i in range(lax.axis_size(axis))])


def owned_waves(rows, owners, index):
    fold = jnp.arange(rows, dtype=jnp.int32)
    return fold * owners + jnp.where(fold % 2 == 0, index, owners - 1 - index)


def coupling_weights(coupling, rows, owners, target, holder):
    fold = jnp.arange(rows, dtype=jnp.int32)
    waves = owned_waves(rows, owners, target)
    totals = [0.0] * 5
    for place, offset in enumerate(OFFSETS):
        wave = waves + offset
        valid = (wave >= 0) & (wave < rows * owners)
        wave = jnp.clip(wave, 0, rows * owners - 1)
        source_fold = wave // owners
        position = wave % owners
        owner = jnp.where(source_fold % 2 == 0, position, owners - 1 - position)
        delta = source_fold - fold
        own = valid & (owner == holder)
        level = valid & (delta == 0)
        picks = (
            own & (delta == -1),
            own & (delta == 0),
            own & (delta == 1),
            level & (owner == holder - 2),
            level & (owner == holder + 2),
        )
        for kind, pick in enumerate(picks):
            totals[kind] = totals[kind] + coupling[place] * pick.astype(jnp.float32)[:, None]
    return totals


def body(forcing, coupling, helmholtz, vertical):
    owners = lax.axis_size("ma")
    index = lax.axis_index("ma")
    partner = index + 1 - 2 * (index % 2)
    levels, _, rows, width = forcing.shape
    all_levels = levels * lax.axis_size("lev")
    start = lax.axis_index("lev") * levels
    weights = lax.dynamic_slice_in_dim(vertical, start, levels, 0)
    diagonal = lax.dynamic_slice_in_dim(jnp.diagonal(vertical), start, levels, 0)
    waves = owned_waves(rows, owners, index)
    positions = jnp.arange(width, dtype=jnp.int32)
    live = (positions[None, :] >= waves[:, None]).astype(jnp.float32)
    scale = 1.0 / (1.0 + helmholtz[None, :] * diagonal[:, None])

    mine = coupling_weights(coupling, rows, owners, index, index)
    theirs = coupling_weights(swapped(coupling, "ma"), rows, owners, partner, index)
    mine = lax.optimization_barrier(jnp.stack(mine))
    theirs = lax.optimization_barrier(jnp.stack(theirs))

    groups = max(width // COLUMN_STEP, 1)
    if width % COLUMN_STEP or rows % groups:
        groups = 1
    size = rows // groups
    solution = jnp.zeros_like(forcing)
    first_sum = jnp.float32(0)
    second_sum = jnp.float32(0)
    sent = []
    for group in range(groups):
        low, left = group * size, group * size * owners
        rhs = forcing[:, :, low : low + size, left:] * live[low : low + size, left:]
        first = lax.optimization_barrier(scale[:, None, None, left:] * rhs)
        below = shifted(first, "ma", 2)
        above = shifted(first, "ma", -2)
        gathered = lax.all_gather(first, "lev", axis=0, tiled=True)
        sent.append((first, below, above, gathered))
    for group in range(groups):
        low, left = group * size, group * size * owners
        first, below, above, gathered = sent[group]
        mask = live[low : low + size, left:]
        rhs = forcing[:, :, low : low + size, left:] * mask
        column_scale = scale[:, None, None, left:]
        empty = jnp.zeros_like(first[:, :, :1])
        before, after = empty, empty
        if group > 0:
            before = sent[group - 1][0][:, :, -1:, size * owners :]
        if group < groups - 1:
            gap = ((0, 0), (0, 0), (0, 0), (size * owners, 0))
            after = jnp.pad(sent[group + 1][0][:, :, :1], gap)
        down = jnp.concatenate([before, first[:, :, :-1]], axis=2)
        up = jnp.concatenate([first[:, :, 1:], after], axis=2)
        fields = (down, first, up, below, above)

        def combined(table):
            part = table[:, low : low + size, left:]
            return sum(part[kind][None, None] * field for kind, field in enumerate(fields))

        received = swapped(combined(theirs), "ma")
        mixed = jnp.einsum("kl,lcin->kcin", weights, gathered, precision=lax.Precision.HIGH)
        result = first + helmholtz[None, None, None, left:] * mixed
        result = result + combined(mine) + received
        residual = rhs - result * mask
        first_sum = first_sum + jnp.sum(rhs * rhs)
        second_sum = second_sum + jnp.sum(residual * residual)
        update = first + column_scale * residual
        solution = lax.dynamic_update_slice(solution, update, (0, 0, low, left))
    sums = lax.psum(jnp.stack([first_sum, second_sum]), ("ma", "lev"))
    norms = jnp.sqrt(sums / (all_levels * width * (width + 1)))
    return (solution, norms)


LANES = 128
SUBLANES = 8
AHEAD = 8
LAG = 3
SEND_SLOTS = 4
MESH = pl.DeviceIdType.MESH


def unit_place(unit, groups):
    pair, step = unit // (groups + 1), unit % (groups + 1)
    far = (step + pair) // groups
    group = pair + far * (groups - 1 - 2 * pair)
    column = (pair + step) * (1 - far) + (step - 1) * far
    return group, column


def tile_weights(coupling, fold, column, owners, target, holder):
    even = (fold & 1) == 0
    place = jnp.where(even, target, owners - 1 - target)
    wave = fold * owners + place
    totals = [jnp.zeros(fold.shape, jnp.float32)] * 5
    for kind, offset in enumerate(OFFSETS):
        moved = place + offset
        delta = jnp.where(moved < 0, -1, jnp.where(moved >= owners, 1, 0))
        position = moved - delta * owners
        parity = (fold + delta) & 1
        owner = jnp.where(parity == 0, position, owners - 1 - position)
        live = (wave + offset >= 0) & (column >= wave + offset)
        value = jnp.where(live, coupling[kind], 0.0)
        where_own = jnp.where(owner == holder, delta, 9)
        where_level = jnp.where(delta == 0, owner - holder, 9)
        picks = (where_own == -1, where_own == 0, where_own == 1, where_level == -2, where_level == 2)
        for i, pick in enumerate(picks):
            totals[i] = totals[i] + jnp.where(pick, value, 0.0)
    return totals


def kernel(
    owners,
    groups,
    forcing,
    coupling,
    scale,
    helmholtz,
    mixing,
    out,
    sums,
    below_in,
    above_in,
    far_in,
    twin_in,
    far_twin_in,
    cross_in,
    weight_in,
    ext,
    low,
    high,
    remote,
    cross,
    mine,
    weights,
    partial,
    result,
    zeros,
    matrix,
    send,
    recv,
    load_sem,
    remote_sem,
    store_sem,
    zero_sem,
):
    levels = forcing.shape[0]
    size = below_in.shape[3]
    units = below_in.shape[0]
    rows = groups * size
    index = lax.axis_index("ma")
    lev = lax.axis_index("lev")
    has_low = index >= 2
    has_high = index < owners - 2
    to_low = {"ma": jnp.maximum(index - 2, 0), "lev": lev}
    to_high = {"ma": jnp.minimum(index + 2, owners - 1), "lev": lev}
    partner = index + 1 - 2 * (index % 2)
    to_cross = {"ma": partner, "lev": lev}
    twin = lev + 1 - 2 * (lev % 2)
    to_twin = {"ma": index, "lev": twin}
    to_far = {"ma": index, "lev": (lev + 2) % 4}
    half = coupling.shape[0] // 2
    part = (lev % 2) * half

    def cut(group, column):
        return pl.ds(pl.multiple_of(group * size, size), size), pl.ds(pl.multiple_of(column * LANES, LANES), LANES)

    def remote_copy(kind, unit, source, target, device):
        return pltpu.make_async_remote_copy(
            src_ref=source,
            dst_ref=target,
            send_sem=send.at[kind, unit],
            recv_sem=recv.at[kind, unit],
            device_id=device,
            device_id_type=MESH,
        )

    def tile(unit):
        group, column = unit_place(unit, groups)
        r, c = cut(group, column)
        return forcing.at[:, :, r, c]

    def copy_high(unit):
        return remote_copy(0, unit, tile(unit), below_in.at[unit], to_high)

    def copy_low(unit):
        return remote_copy(1, unit, tile(unit), above_in.at[unit], to_low)

    def copy_far(unit):
        return remote_copy(2, unit, tile(unit), far_in.at[unit], to_far)

    def copy_twin(unit):
        return remote_copy(3, unit, tile(unit), twin_in.at[unit], to_twin)

    def copy_far_twin(unit):
        return remote_copy(4, unit, far_in.at[unit], far_twin_in.at[unit], to_twin)

    def copy_cross(unit):
        return remote_copy(5, unit, partial.at[unit % SEND_SLOTS], cross_in.at[unit], to_cross)

    def copy_weight(unit):
        group, column = unit_place(unit, groups)
        r, c = cut(group, column)
        source = coupling.at[pl.ds(part, half), r, c]
        return remote_copy(6, unit, source, weight_in.at[unit, pl.ds(part, half)], to_cross)

    def copy_weight_twin(unit):
        held = weight_in.at[unit, pl.ds(part, half)]
        return remote_copy(7, unit, held, held, to_twin)

    def wait_weight_twin(unit):
        held = weight_in.at[unit, pl.ds(half - part, half)]
        remote_copy(7, unit, held, held, to_twin).wait_recv()

    def start_sends(unit):
        @pl.when(has_high)
        def _():
            copy_high(unit).start()

        @pl.when(has_low)
        def _():
            copy_low(unit).start()

        copy_weight(unit).start()
        copy_far(unit).start()
        copy_twin(unit).start()

    def near_loads(unit):
        group, column = unit_place(unit, groups)
        r, c = cut(group, column)
        slot = unit % (LAG + 1)
        first = group * size
        ahead = pl.ds(pl.multiple_of(jnp.maximum(first - SUBLANES, 0), SUBLANES), SUBLANES)
        behind = pl.ds(pl.multiple_of(jnp.minimum(first + size, rows - SUBLANES), SUBLANES), SUBLANES)
        return [
            pltpu.make_async_copy(forcing.at[:, :, ahead, c], ext.at[slot, :, :, pl.ds(0, SUBLANES)], load_sem.at[0]),
            pltpu.make_async_copy(forcing.at[:, :, r, c], ext.at[slot, :, :, pl.ds(SUBLANES, size)], load_sem.at[1]),
            pltpu.make_async_copy(forcing.at[:, :, behind, c], ext.at[slot, :, :, pl.ds(SUBLANES + size, SUBLANES)], load_sem.at[2]),
            pltpu.make_async_copy(coupling.at[:, r, c], weights.at[0], load_sem.at[3]),
        ]

    def low_load(unit):
        return pltpu.make_async_copy(below_in.at[unit], low, load_sem.at[4])

    def high_load(unit):
        return pltpu.make_async_copy(above_in.at[unit], high, load_sem.at[5])

    def weight_load(unit):
        return pltpu.make_async_copy(weight_in.at[unit], weights.at[1], load_sem.at[6])

    def remote_loads(unit):
        return [
            pltpu.make_async_copy(twin_in.at[unit], remote.at[0], remote_sem.at[0]),
            pltpu.make_async_copy(far_in.at[unit], remote.at[1], remote_sem.at[1]),
            pltpu.make_async_copy(far_twin_in.at[unit], remote.at[2], remote_sem.at[2]),
            pltpu.make_async_copy(cross_in.at[unit], cross, remote_sem.at[3]),
        ]

    def store(unit):
        group, column = unit_place(unit, groups)
        r, c = cut(group, column)
        return pltpu.make_async_copy(result.at[unit % 2], out.at[:, :, r, c], store_sem.at[unit % 2])

    def zero_store(unit):
        pair, step = unit // (groups + 1), unit % (groups + 1)
        far = jnp.where(step < pair, 0, 1)
        group = pair + far * (groups - 1 - 2 * pair)
        column = step - far * pair
        r, c = cut(group, column)
        return pltpu.make_async_copy(zeros, out.at[:, :, r, c], zero_sem.at[0])

    def has_zero(unit):
        return (unit >= 0) & (unit < units) & (unit % (groups + 1) < groups - 1)

    def near_step(unit):
        group, column = unit_place(unit, groups)
        slot = unit % (LAG + 1)
        fold = group * size + lax.broadcasted_iota(jnp.int32, (size, LANES), 0)
        lane = column * LANES + lax.broadcasted_iota(jnp.int32, (size, LANES), 1)
        own = tile_weights(weights[0], fold, lane, owners, index, index)
        theirs = tile_weights(weights[1], fold, lane, owners, partner, index)
        for c in range(2):
            fields = (
                ext[slot, :, c, SUBLANES - 1 : SUBLANES - 1 + size, :],
                ext[slot, :, c, SUBLANES : SUBLANES + size, :],
                ext[slot, :, c, SUBLANES + 1 : SUBLANES + 1 + size, :],
                low[:, c],
                high[:, c],
            )
            mine[slot, :, c] = sum(w[None] * f for w, f in zip(own, fields))
            partial[unit % SEND_SLOTS, :, c] = sum(w[None] * f for w, f in zip(theirs, fields))

    def final_step(unit):
        group, column = unit_place(unit, groups)
        slot = unit % (LAG + 1)
        scales = scale[column]
        own_scale = scales[:levels]
        helm = helmholtz[column][None]
        for tall in range(size // SUBLANES):
            start = tall * SUBLANES
            for c in range(2):
                lanes = pl.ds(c * LANES, LANES)
                for source in range(4):
                    if source == 0:
                        raw = ext[slot, :, c, SUBLANES + start : 2 * SUBLANES + start, :]
                    else:
                        raw = remote[source - 1, :, c, start : start + SUBLANES, :]
                    value = raw * scales[source * levels : (source + 1) * levels]
                    value = value.reshape(levels * SUBLANES, LANES)
                    coarse = value.astype(jnp.bfloat16)
                    fine = (value - coarse.astype(jnp.float32)).astype(jnp.bfloat16)
                    span = pl.ds(source * levels * SUBLANES, levels * SUBLANES)
                    matrix[0, span, lanes] = coarse
                    matrix[1, span, lanes] = fine
            depth = levels * SUBLANES
            both = jnp.dot(mixing[...], matrix[0], preferred_element_type=jnp.float32)
            rest = jnp.dot(mixing[:depth], matrix[1], preferred_element_type=jnp.float32)
            total = both[:depth] + both[depth:] + rest
            fold = group * size + start + lax.broadcasted_iota(jnp.int32, (SUBLANES, LANES), 0)
            lane = column * LANES + lax.broadcasted_iota(jnp.int32, (SUBLANES, LANES), 1)
            place = jnp.where((fold & 1) == 0, index, owners - 1 - index)
            mask = (lane >= fold * owners + place).astype(jnp.float32)[None]
            for c in range(2):
                mixed = total[:, c * LANES : (c + 1) * LANES].reshape(levels, SUBLANES, LANES)
                rhs = ext[slot, :, c, SUBLANES + start : 2 * SUBLANES + start, :] * mask
                first = own_scale * rhs
                near = mine[slot, :, c, start : start + SUBLANES, :] + cross[:, c, start : start + SUBLANES, :]
                applied = first + helm * mixed + own_scale * near
                residual = rhs - applied * mask
                result[unit % 2, :, c, start : start + SUBLANES, :] = first + own_scale * residual
                sums[0] += jnp.sum(rhs * rhs, axis=0)
                sums[1] += jnp.sum(residual * residual, axis=0)

    barrier = pltpu.get_barrier_semaphore()
    for device in (to_cross, to_twin, to_far):
        pl.semaphore_signal(barrier, inc=1, device_id=device, device_id_type=MESH)

    @pl.when(has_low)
    def _():
        pl.semaphore_signal(barrier, inc=1, device_id=to_low, device_id_type=MESH)

    @pl.when(has_high)
    def _():
        pl.semaphore_signal(barrier, inc=1, device_id=to_high, device_id_type=MESH)

    pl.semaphore_wait(barrier, 3 + jnp.where(has_low, 1, 0) + jnp.where(has_high, 1, 0))

    def begin(unit, carry):
        start_sends(unit)
        return carry

    lax.fori_loop(0, min(AHEAD, units), begin, 0)
    zeros[...] = jnp.zeros_like(zeros)
    sums[...] = jnp.zeros_like(sums)

    def step(now, carry):
        @pl.when(now + AHEAD < units)
        def _():
            start_sends(now + AHEAD)

        @pl.when(has_zero(now - 1))
        def _():
            zero_store(now - 1).wait()

        @pl.when(has_zero(now))
        def _():
            zero_store(now).start()

        @pl.when(now < units)
        def _():
            for copy in near_loads(now):
                copy.start()
            copy_weight(now).wait()
            copy_weight_twin(now).start()

            @pl.when(has_low)
            def _():
                copy_high(now).wait_recv()
                low_load(now).start()

            @pl.when(jnp.logical_not(has_low))
            def _():
                pltpu.make_async_copy(tile(now), low, load_sem.at[4]).start()

            @pl.when(has_high)
            def _():
                copy_low(now).wait_recv()
                high_load(now).start()

            @pl.when(jnp.logical_not(has_high))
            def _():
                pltpu.make_async_copy(tile(now), high, load_sem.at[5]).start()

            copy_far(now).wait()
            copy_far_twin(now).start()
            wait_weight_twin(now)
            weight_load(now).start()

        @pl.when(now >= LAG)
        def _():
            unit = now - LAG
            for copy in remote_loads(unit):
                copy.wait()

            @pl.when(unit >= 2)
            def _():
                store(unit - 2).wait()

            final_step(unit)
            store(unit).start()

        @pl.when(now < units)
        def _():
            for copy in near_loads(now):
                copy.wait()
            low_load(now).wait()
            high_load(now).wait()
            weight_load(now).wait()

            @pl.when(now >= SEND_SLOTS)
            def _():
                copy_cross(now - SEND_SLOTS).wait_send()

            near_step(now)
            copy_cross(now).start()

            @pl.when(has_high)
            def _():
                copy_high(now).wait_send()

            @pl.when(has_low)
            def _():
                copy_low(now).wait_send()

        @pl.when((now >= LAG - 1) & (now < units + LAG - 1))
        def _():
            unit = now - (LAG - 1)
            copy_twin(unit).wait()
            copy_far_twin(unit).wait()
            copy_weight_twin(unit).wait_send()
            copy_cross(unit).wait_recv()
            for copy in remote_loads(unit):
                copy.start()

        return carry

    lax.fori_loop(0, units + LAG, step, 0)
    for unit in range(max(units - SEND_SLOTS, 0), units):
        copy_cross(unit).wait_send()
    for unit in range(max(units - 2, 0), units):
        store(unit).wait()


def kernel_body(forcing, coupling, helmholtz, vertical):
    owners = lax.axis_size("ma")
    levels, parts, rows, width = forcing.shape
    lev = lax.axis_index("lev")
    size = LANES // owners
    groups = rows // size
    units = groups * (groups + 1) // 2
    blocks = [lev, lev + 1 - 2 * (lev % 2)]
    blocks = blocks + [(block + 2) % 4 for block in blocks]
    own = lax.dynamic_slice_in_dim(vertical, lev * levels, levels, 0)
    mixing = jnp.concatenate([lax.dynamic_slice_in_dim(own, block * levels, levels, 1) for block in blocks], axis=1)
    diagonal = jnp.diagonal(vertical)
    diagonal = jnp.concatenate([lax.dynamic_slice_in_dim(diagonal, block * levels, levels, 0) for block in blocks])
    scale = 1.0 / (1.0 + helmholtz.reshape(groups, 1, LANES) * diagonal[None, :, None])
    scale = scale[:, :, None, :]
    eye = jnp.eye(SUBLANES, dtype=jnp.float32)
    wide = (mixing[:, None, :, None] * eye[None, :, None, :]).reshape(levels * SUBLANES, 4 * levels * SUBLANES)
    coarse = lax.reduce_precision(wide, 8, 7)
    mixing = jnp.concatenate([coarse, wide - coarse], axis=0).astype(jnp.bfloat16)
    block = (levels, parts, size, LANES)
    kinds = coupling.shape[0]
    f32 = jnp.float32
    slab = jax.ShapeDtypeStruct((units,) + block, f32)
    anywhere = pl.BlockSpec(memory_space=pl.ANY)
    vmem = pl.BlockSpec(memory_space=pltpu.VMEM)
    ext = (LAG + 1, levels, parts, size + 2 * SUBLANES, LANES)
    results = pl.pallas_call(
        functools.partial(kernel, owners, groups),
        out_shape=[
            jax.ShapeDtypeStruct(forcing.shape, f32),
            jax.ShapeDtypeStruct((2, SUBLANES, LANES), f32),
            slab,
            slab,
            slab,
            slab,
            slab,
            slab,
            jax.ShapeDtypeStruct((units, kinds, size, LANES), f32),
        ],
        in_specs=[anywhere, anywhere, vmem, vmem, vmem],
        out_specs=[anywhere, vmem] + [anywhere] * 7,
        scratch_shapes=[
            pltpu.VMEM(ext, f32),
            pltpu.VMEM(block, f32),
            pltpu.VMEM(block, f32),
            pltpu.VMEM((3,) + block, f32),
            pltpu.VMEM(block, f32),
            pltpu.VMEM((LAG + 1,) + block, f32),
            pltpu.VMEM((2, kinds, size, LANES), f32),
            pltpu.VMEM((SEND_SLOTS,) + block, f32),
            pltpu.VMEM((2,) + block, f32),
            pltpu.VMEM(block, f32),
            pltpu.VMEM((2, 4 * levels * SUBLANES, parts * LANES), jnp.bfloat16),
            pltpu.SemaphoreType.DMA((8, units)),
            pltpu.SemaphoreType.DMA((8, units)),
            pltpu.SemaphoreType.DMA((7,)),
            pltpu.SemaphoreType.DMA((4,)),
            pltpu.SemaphoreType.DMA((2,)),
            pltpu.SemaphoreType.DMA((1,)),
        ],
        compiler_params=pltpu.CompilerParams(collective_id=0, has_side_effects=True, vmem_limit_bytes=48 * 2**20),
        name="richardson",
    )(forcing, coupling, scale, helmholtz.reshape(groups, 1, LANES), mixing)
    total = lax.psum(jnp.sum(results[1], axis=(1, 2)), ("ma", "lev"))
    norms = jnp.sqrt(total / (4 * levels * width * (width + 1)))
    return (results[0], norms)


def fits_kernel(forcing, coupling):
    owners, levs = lax.axis_size("ma"), lax.axis_size("lev")
    rows, width = forcing.shape[2:]
    whole = LANES % owners == 0 and (LANES // owners) % SUBLANES == 0
    return whole and levs == 4 and owners >= 4 and width == rows * owners and width % (2 * LANES) == 0


def device_body(forcing, coupling, helmholtz, vertical):
    run = kernel_body if fits_kernel(forcing, coupling) else body
    return run(forcing, coupling, helmholtz, vertical)


def solution(mesh):
    in_specs = (P("lev", None, "ma", None), P(None, "ma", None), P(), P())
    out_specs = (P("lev", None, "ma", None), P())
    return jax.shard_map(device_body, mesh=mesh, in_specs=in_specs, out_specs=out_specs, check_vma=False)
```

```python
import functools

import jax
import jax.numpy as jnp
from jax import lax
from jax.experimental import pallas as pl
from jax.experimental.pallas import tpu as pltpu
from jax.sharding import PartitionSpec as P

OFFSETS = (-2, -1, 1, 2)
COLUMN_STEP = 256


def shifted(block, axis, distance):
    devices = range(lax.axis_size(axis))
    route = [(i - distance, i) for i in devices if i - distance in devices]
    return lax.ppermute(block, axis, route)


def swapped(block, axis):
    return lax.ppermute(block, axis, [(i, i ^ 1) for i in range(lax.axis_size(axis))])


def owned_waves(rows, owners, index):
    fold = jnp.arange(rows, dtype=jnp.int32)
    return fold * owners + jnp.where(fold % 2 == 0, index, owners - 1 - index)


def coupling_weights(coupling, rows, owners, target, holder):
    fold = jnp.arange(rows, dtype=jnp.int32)
    waves = owned_waves(rows, owners, target)
    totals = [0.0] * 5
    for place, offset in enumerate(OFFSETS):
        wave = waves + offset
        valid = (wave >= 0) & (wave < rows * owners)
        wave = jnp.clip(wave, 0, rows * owners - 1)
        source_fold = wave // owners
        position = wave % owners
        owner = jnp.where(source_fold % 2 == 0, position, owners - 1 - position)
        delta = source_fold - fold
        own = valid & (owner == holder)
        level = valid & (delta == 0)
        picks = (
            own & (delta == -1),
            own & (delta == 0),
            own & (delta == 1),
            level & (owner == holder - 2),
            level & (owner == holder + 2),
        )
        for kind, pick in enumerate(picks):
            totals[kind] = totals[kind] + coupling[place] * pick.astype(jnp.float32)[:, None]
    return totals


def body(forcing, coupling, helmholtz, vertical):
    owners = lax.axis_size("ma")
    index = lax.axis_index("ma")
    partner = index + 1 - 2 * (index % 2)
    levels, _, rows, width = forcing.shape
    all_levels = levels * lax.axis_size("lev")
    start = lax.axis_index("lev") * levels
    weights = lax.dynamic_slice_in_dim(vertical, start, levels, 0)
    diagonal = lax.dynamic_slice_in_dim(jnp.diagonal(vertical), start, levels, 0)
    waves = owned_waves(rows, owners, index)
    positions = jnp.arange(width, dtype=jnp.int32)
    live = (positions[None, :] >= waves[:, None]).astype(jnp.float32)
    scale = 1.0 / (1.0 + helmholtz[None, :] * diagonal[:, None])

    mine = coupling_weights(coupling, rows, owners, index, index)
    theirs = coupling_weights(swapped(coupling, "ma"), rows, owners, partner, index)
    mine = lax.optimization_barrier(jnp.stack(mine))
    theirs = lax.optimization_barrier(jnp.stack(theirs))

    groups = max(width // COLUMN_STEP, 1)
    if width % COLUMN_STEP or rows % groups:
        groups = 1
    size = rows // groups
    solution = jnp.zeros_like(forcing)
    first_sum = jnp.float32(0)
    second_sum = jnp.float32(0)
    sent = []
    for group in range(groups):
        low, left = group * size, group * size * owners
        rhs = forcing[:, :, low : low + size, left:] * live[low : low + size, left:]
        first = lax.optimization_barrier(scale[:, None, None, left:] * rhs)
        below = shifted(first, "ma", 2)
        above = shifted(first, "ma", -2)
        gathered = lax.all_gather(first, "lev", axis=0, tiled=True)
        sent.append((first, below, above, gathered))
    for group in range(groups):
        low, left = group * size, group * size * owners
        first, below, above, gathered = sent[group]
        mask = live[low : low + size, left:]
        rhs = forcing[:, :, low : low + size, left:] * mask
        column_scale = scale[:, None, None, left:]
        empty = jnp.zeros_like(first[:, :, :1])
        before, after = empty, empty
        if group > 0:
            before = sent[group - 1][0][:, :, -1:, size * owners :]
        if group < groups - 1:
            gap = ((0, 0), (0, 0), (0, 0), (size * owners, 0))
            after = jnp.pad(sent[group + 1][0][:, :, :1], gap)
        down = jnp.concatenate([before, first[:, :, :-1]], axis=2)
        up = jnp.concatenate([first[:, :, 1:], after], axis=2)
        fields = (down, first, up, below, above)

        def combined(table):
            part = table[:, low : low + size, left:]
            return sum(part[kind][None, None] * field for kind, field in enumerate(fields))

        received = swapped(combined(theirs), "ma")
        mixed = jnp.einsum("kl,lcin->kcin", weights, gathered, precision=lax.Precision.HIGH)
        result = first + helmholtz[None, None, None, left:] * mixed
        result = result + combined(mine) + received
        residual = rhs - result * mask
        first_sum = first_sum + jnp.sum(rhs * rhs)
        second_sum = second_sum + jnp.sum(residual * residual)
        update = first + column_scale * residual
        solution = lax.dynamic_update_slice(solution, update, (0, 0, low, left))
    sums = lax.psum(jnp.stack([first_sum, second_sum]), ("ma", "lev"))
    norms = jnp.sqrt(sums / (all_levels * width * (width + 1)))
    return (solution, norms)


LANES = 128
SUBLANES = 8
AHEAD = 6
WEIGHT_AHEAD = 20
WHOLE = 10
RELAY_AHEAD = 12
JOIN_AHEAD = 2
LAG = 3
SEND_SLOTS = 4
MESH = pl.DeviceIdType.MESH


def unit_place(unit, groups):
    pair, step = unit // (groups + 1), unit % (groups + 1)
    far = (step + pair) // groups
    group = pair + far * (groups - 1 - 2 * pair)
    column = (pair + step) * (1 - far) + (step - 1) * far
    return group, column


def tile_weights(coupling, fold, column, owners, target, holder):
    even = (fold & 1) == 0
    place = jnp.where(even, target, owners - 1 - target)
    wave = fold * owners + place
    totals = [jnp.zeros(fold.shape, jnp.float32)] * 5
    for kind, offset in enumerate(OFFSETS):
        moved = place + offset
        delta = jnp.where(moved < 0, -1, jnp.where(moved >= owners, 1, 0))
        position = moved - delta * owners
        parity = (fold + delta) & 1
        owner = jnp.where(parity == 0, position, owners - 1 - position)
        live = (wave + offset >= 0) & (column >= wave + offset)
        value = jnp.where(live, coupling[kind], 0.0)
        where_own = jnp.where(owner == holder, delta, 9)
        where_level = jnp.where(delta == 0, owner - holder, 9)
        picks = (where_own == -1, where_own == 0, where_own == 1, where_level == -2, where_level == 2)
        for i, pick in enumerate(picks):
            totals[i] = totals[i] + jnp.where(pick, value, 0.0)
    return totals


def prepare(vertical, helmholtz, mixing, scale, blocks, levels):
    total = vertical.shape[0]
    depth, full = levels * SUBLANES, total * SUBLANES
    bits = SUBLANES.bit_length() - 1

    def iota(shape, axis):
        return lax.broadcasted_iota(jnp.int32, shape, axis)

    def one_hot(pick):
        return jnp.where(pick, 1.0, 0.0).astype(jnp.bfloat16)

    values = vertical[...]
    coarse = values.astype(jnp.bfloat16)
    fine = (values - coarse.astype(jnp.float32)).astype(jnp.bfloat16)
    pick = one_hot((iota((depth, total), 0) >> bits) + blocks[0] * levels == iota((depth, total), 1))
    level = iota((total, full), 1) >> bits
    source = level + blocks[0] * levels
    for i, block in enumerate(blocks):
        source = jnp.where(level >= i * levels, level + (block - i) * levels, source)
    spread = one_hot(source == iota((total, full), 0))
    same = (iota((depth, full), 0) & (SUBLANES - 1)) == (iota((depth, full), 1) & (SUBLANES - 1))
    for i, part in enumerate((coarse, fine)):
        chosen = jnp.dot(pick, part, preferred_element_type=jnp.float32).astype(jnp.bfloat16)
        wide = jnp.dot(chosen, spread, preferred_element_type=jnp.float32)
        mixing[pl.ds(i * depth, depth)] = jnp.where(same, wide, 0.0).astype(jnp.bfloat16)
    here = iota((total, total), 0) == iota((total, total), 1)
    diagonal = jnp.sum(jnp.where(here, values, 0.0), axis=1, keepdims=True)
    diagonal = jnp.broadcast_to(diagonal, (total, LANES))[:, None, :]
    for column in range(scale.shape[0]):
        scale[column] = 1.0 / (1.0 + helmholtz[column][None] * diagonal)


def kernel(
    owners,
    groups,
    forcing,
    coupling,
    helmholtz,
    vertical,
    out,
    sums,
    below_in,
    above_in,
    far_in,
    twin_in,
    far_twin_in,
    cross_in,
    weight_in,
    scale,
    mixing,
    ext,
    low,
    high,
    remote,
    cross,
    mine,
    weights,
    partial,
    result,
    matrix,
    total_out,
    total_in,
    send,
    recv,
    load_sem,
    remote_sem,
    store_sem,
    sum_send,
    sum_recv,
):
    levels = forcing.shape[0]
    size = below_in.shape[3]
    units = below_in.shape[0]
    rows = groups * size
    index = lax.axis_index("ma")
    lev = lax.axis_index("lev")
    has_low = index >= 2
    has_high = index < owners - 2
    to_low = {"ma": jnp.maximum(index - 2, 0), "lev": lev}
    to_high = {"ma": jnp.minimum(index + 2, owners - 1), "lev": lev}
    partner = index + 1 - 2 * (index % 2)
    to_cross = {"ma": partner, "lev": lev}
    twin = lev + 1 - 2 * (lev % 2)
    far = (lev + 2) % 4
    far_twin = (twin + 2) % 4
    to_twin = {"ma": index, "lev": twin}
    to_far = {"ma": index, "lev": far}
    share = coupling.shape[0] // 4
    span = owners // 2
    spans = []
    while span >= 4:
        spans.append(span)
        span //= 2
    to_spans = [{"ma": index + span - 2 * span * ((index // span) % 2), "lev": lev} for span in spans]
    to_pair = {"ma": index + 2 - 4 * ((index // 2) % 2), "lev": lev}

    def cut(group, column):
        return pl.ds(pl.multiple_of(group * size, size), size), pl.ds(pl.multiple_of(column * LANES, LANES), LANES)

    def remote_copy(kind, unit, source, target, device):
        return pltpu.make_async_remote_copy(
            src_ref=source,
            dst_ref=target,
            send_sem=send.at[kind, unit],
            recv_sem=recv.at[kind, unit],
            device_id=device,
            device_id_type=MESH,
        )

    def tile(unit):
        group, column = unit_place(unit, groups)
        r, c = cut(group, column)
        return forcing.at[:, :, r, c]

    def copy_high(unit):
        return remote_copy(0, unit, tile(unit), below_in.at[unit], to_high)

    def copy_low(unit):
        return remote_copy(1, unit, tile(unit), above_in.at[unit], to_low)

    def copy_far(unit):
        return remote_copy(2, unit, tile(unit), far_in.at[unit], to_far)

    def copy_twin(unit):
        return remote_copy(3, unit, tile(unit), twin_in.at[unit], to_twin)

    def copy_far_twin(unit):
        return remote_copy(4, unit, far_in.at[unit], far_twin_in.at[unit], to_twin)

    def copy_cross(unit):
        return remote_copy(5, unit, partial.at[unit % SEND_SLOTS], cross_in.at[unit], to_cross)

    def held(unit, owner):
        return weight_in.at[unit, pl.ds(owner * share, share)]

    def copy_weight(unit):
        group, column = unit_place(unit, groups)
        r, c = cut(group, column)
        source = coupling.at[pl.ds(lev * share, share), r, c]
        return remote_copy(6, unit, source, held(unit, lev), to_cross)

    def copy_weights(unit):
        group, column = unit_place(unit, groups)
        r, c = cut(group, column)
        return remote_copy(6, unit, coupling.at[:, r, c], weight_in.at[unit], to_cross)

    def relay_twin(unit):
        return remote_copy(7, unit, held(unit, lev), held(unit, lev), to_twin)

    def relay_far(unit):
        return remote_copy(8, unit, held(unit, lev), held(unit, lev), to_far)

    def relay_far_twin(unit):
        return remote_copy(9, unit, held(unit, far), held(unit, far), to_twin)

    def from_twin(unit):
        return remote_copy(7, unit, held(unit, twin), held(unit, twin), to_twin)

    def from_far(unit):
        return remote_copy(8, unit, held(unit, far), held(unit, far), to_far)

    def from_far_twin(unit):
        return remote_copy(9, unit, held(unit, far_twin), held(unit, far_twin), to_twin)

    def start_sends(unit):
        @pl.when(has_high)
        def _():
            copy_high(unit).start()

        @pl.when(has_low)
        def _():
            copy_low(unit).start()

        copy_far(unit).start()
        copy_twin(unit).start()

    def near_loads(unit):
        group, column = unit_place(unit, groups)
        r, c = cut(group, column)
        slot = unit % (LAG + 1)
        first = group * size
        ahead = pl.ds(pl.multiple_of(jnp.maximum(first - SUBLANES, 0), SUBLANES), SUBLANES)
        behind = pl.ds(pl.multiple_of(jnp.minimum(first + size, rows - SUBLANES), SUBLANES), SUBLANES)
        return [
            pltpu.make_async_copy(forcing.at[:, :, ahead, c], ext.at[slot, :, :, pl.ds(0, SUBLANES)], load_sem.at[0]),
            pltpu.make_async_copy(forcing.at[:, :, r, c], ext.at[slot, :, :, pl.ds(SUBLANES, size)], load_sem.at[1]),
            pltpu.make_async_copy(forcing.at[:, :, behind, c], ext.at[slot, :, :, pl.ds(SUBLANES + size, SUBLANES)], load_sem.at[2]),
            pltpu.make_async_copy(coupling.at[:, r, c], weights.at[0], load_sem.at[3]),
        ]

    def low_load(unit):
        return pltpu.make_async_copy(below_in.at[unit], low, load_sem.at[4])

    def high_load(unit):
        return pltpu.make_async_copy(above_in.at[unit], high, load_sem.at[5])

    def weight_load(unit):
        return pltpu.make_async_copy(weight_in.at[unit], weights.at[1], load_sem.at[6])

    def remote_loads(unit):
        return [
            pltpu.make_async_copy(twin_in.at[unit], remote.at[0], remote_sem.at[0]),
            pltpu.make_async_copy(far_in.at[unit], remote.at[1], remote_sem.at[1]),
            pltpu.make_async_copy(far_twin_in.at[unit], remote.at[2], remote_sem.at[2]),
            pltpu.make_async_copy(cross_in.at[unit], cross, remote_sem.at[3]),
        ]

    def store(unit):
        return pltpu.make_async_copy(result.at[unit % 2], out.at[unit], store_sem.at[unit % 2])

    def near_step(unit):
        group, column = unit_place(unit, groups)
        slot = unit % (LAG + 1)
        fold = group * size + lax.broadcasted_iota(jnp.int32, (size, LANES), 0)
        lane = column * LANES + lax.broadcasted_iota(jnp.int32, (size, LANES), 1)
        own = tile_weights(weights[0], fold, lane, owners, index, index)
        theirs = tile_weights(weights[1], fold, lane, owners, partner, index)
        for c in range(2):
            fields = (
                ext[slot, :, c, SUBLANES - 1 : SUBLANES - 1 + size, :],
                ext[slot, :, c, SUBLANES : SUBLANES + size, :],
                ext[slot, :, c, SUBLANES + 1 : SUBLANES + 1 + size, :],
                low[:, c],
                high[:, c],
            )
            mine[slot, :, c] = sum(w[None] * f for w, f in zip(own, fields))
            partial[unit % SEND_SLOTS, :, c] = sum(w[None] * f for w, f in zip(theirs, fields))

    def final_step(unit):
        group, column = unit_place(unit, groups)
        slot = unit % (LAG + 1)
        own_scale = scale[column, pl.ds(lev * levels, levels)]
        helm = helmholtz[column][None]
        for tall in range(size // SUBLANES):
            start = tall * SUBLANES
            for c in range(2):
                lanes = pl.ds(c * LANES, LANES)
                for source, block in enumerate((lev, twin, far, far_twin)):
                    if source == 0:
                        raw = ext[slot, :, c, SUBLANES + start : 2 * SUBLANES + start, :]
                    else:
                        raw = remote[source - 1, :, c, start : start + SUBLANES, :]
                    value = raw * scale[column, pl.ds(block * levels, levels)]
                    value = value.reshape(levels * SUBLANES, LANES)
                    coarse = value.astype(jnp.bfloat16)
                    fine = (value - coarse.astype(jnp.float32)).astype(jnp.bfloat16)
                    depth = levels * SUBLANES
                    rows_of = pl.ds(source * depth, depth)
                    matrix[0, rows_of, lanes] = coarse
                    matrix[1, rows_of, lanes] = fine
            both = jnp.dot(mixing[...], matrix[0], preferred_element_type=jnp.float32)
            rest = jnp.dot(mixing[:depth], matrix[1], preferred_element_type=jnp.float32)
            total = both[:depth] + both[depth:] + rest
            fold = group * size + start + lax.broadcasted_iota(jnp.int32, (SUBLANES, LANES), 0)
            lane = column * LANES + lax.broadcasted_iota(jnp.int32, (SUBLANES, LANES), 1)
            place = jnp.where((fold & 1) == 0, index, owners - 1 - index)
            mask = (lane >= fold * owners + place).astype(jnp.float32)[None]
            for c in range(2):
                mixed = total[:, c * LANES : (c + 1) * LANES].reshape(levels, SUBLANES, LANES)
                rhs = ext[slot, :, c, SUBLANES + start : 2 * SUBLANES + start, :] * mask
                first = own_scale * rhs
                near = mine[slot, :, c, start : start + SUBLANES, :] + cross[:, c, start : start + SUBLANES, :]
                applied = first + helm * mixed + own_scale * near
                residual = rhs - applied * mask
                result[unit % 2, :, c, start : start + SUBLANES, :] = first + own_scale * residual
                sums[0] += jnp.sum(rhs * rhs, axis=0)
                sums[1] += jnp.sum(residual * residual, axis=0)

    barrier = pltpu.get_barrier_semaphore()
    for device in [to_cross, to_twin, to_far] + to_spans:
        pl.semaphore_signal(barrier, inc=1, device_id=device, device_id_type=MESH)

    @pl.when(has_low)
    def _():
        pl.semaphore_signal(barrier, inc=1, device_id=to_low, device_id_type=MESH)

    @pl.when(has_high)
    def _():
        pl.semaphore_signal(barrier, inc=1, device_id=to_high, device_id_type=MESH)

    pl.semaphore_wait(barrier, 3 + len(spans) + jnp.where(has_low, 1, 0) + jnp.where(has_high, 1, 0))

    def begin(unit, carry):
        start_sends(unit)
        return carry

    def begin_weights(unit, carry):
        copy_weights(unit).start()
        return carry

    def begin_weight(unit, carry):
        copy_weight(unit).start()
        return carry

    whole = min(WHOLE, units)
    lax.fori_loop(0, min(AHEAD, units), begin, 0)
    lax.fori_loop(0, whole, begin_weights, 0)
    lax.fori_loop(whole, min(WEIGHT_AHEAD, units), begin_weight, 0)
    sums[...] = jnp.zeros_like(sums)
    prepare(vertical, helmholtz, mixing, scale, (lev, twin, far, far_twin), levels)

    def relay(unit, carry):
        copy_weight(unit).wait()
        relay_twin(unit).start()
        relay_far(unit).start()
        return carry

    lax.fori_loop(whole, min(RELAY_AHEAD, units), relay, 0)

    def step(now, carry):
        @pl.when(now + AHEAD < units)
        def _():
            start_sends(now + AHEAD)

        @pl.when(now + WEIGHT_AHEAD < units)
        def _():
            copy_weight(now + WEIGHT_AHEAD).start()

        @pl.when(now < units)
        def _():
            for copy in near_loads(now):
                copy.start()

        @pl.when(now + RELAY_AHEAD < units)
        def _():
            relay(now + RELAY_AHEAD, 0)

        @pl.when((now + JOIN_AHEAD >= whole) & (now + JOIN_AHEAD < units))
        def _():
            unit = now + JOIN_AHEAD
            from_far(unit).wait_recv()
            relay_far_twin(unit).start()

        @pl.when(now < whole)
        def _():
            copy_weights(now).wait()

        @pl.when((now >= whole) & (now < units))
        def _():
            from_twin(now).wait_recv()
            from_far_twin(now).wait_recv()

        @pl.when(now < units)
        def _():
            weight_load(now).start()

            @pl.when(has_low)
            def _():
                copy_high(now).wait_recv()
                low_load(now).start()

            @pl.when(jnp.logical_not(has_low))
            def _():
                pltpu.make_async_copy(tile(now), low, load_sem.at[4]).start()

            @pl.when(has_high)
            def _():
                copy_low(now).wait_recv()
                high_load(now).start()

            @pl.when(jnp.logical_not(has_high))
            def _():
                pltpu.make_async_copy(tile(now), high, load_sem.at[5]).start()

        @pl.when(now >= LAG)
        def _():
            unit = now - LAG
            for copy in remote_loads(unit):
                copy.wait()

            @pl.when(unit >= 2)
            def _():
                store(unit - 2).wait()

            final_step(unit)
            store(unit).start()

        @pl.when(now < units)
        def _():
            for copy in near_loads(now):
                copy.wait()
            low_load(now).wait()
            high_load(now).wait()
            weight_load(now).wait()

            @pl.when(now >= SEND_SLOTS)
            def _():
                copy_cross(now - SEND_SLOTS).wait_send()

            near_step(now)
            copy_cross(now).start()
            copy_far(now).wait()
            copy_far_twin(now).start()

            @pl.when(has_high)
            def _():
                copy_high(now).wait_send()

            @pl.when(has_low)
            def _():
                copy_low(now).wait_send()


        @pl.when((now >= whole) & (now < units))
        def _():
            relay_twin(now).wait_send()
            relay_far(now).wait_send()
            relay_far_twin(now).wait_send()

        @pl.when((now >= LAG - 1) & (now < units + LAG - 1))
        def _():
            unit = now - (LAG - 1)
            copy_twin(unit).wait()
            copy_far_twin(unit).wait()
            copy_cross(unit).wait_recv()
            for copy in remote_loads(unit):
                copy.start()

        return carry

    lax.fori_loop(0, units + LAG, step, 0)
    for unit in range(max(units - SEND_SLOTS, 0), units):
        copy_cross(unit).wait_send()
    peers = [to_twin, to_far, to_cross, to_pair] + to_spans
    total_out[0] = sums[...]
    for i, device in enumerate(peers):
        exchange = pltpu.make_async_remote_copy(
            src_ref=total_out.at[i],
            dst_ref=total_in.at[i],
            send_sem=sum_send.at[i],
            recv_sem=sum_recv.at[i],
            device_id=device,
            device_id_type=MESH,
        )
        exchange.start()
        exchange.wait()
        joined = total_out[i] + total_in[i]
        if i + 1 < len(peers):
            total_out[i + 1] = joined
        else:
            sums[...] = joined
    for unit in range(max(units - 2, 0), units):
        store(unit).wait()


def spread_kernel(groups, packed, out, held, zeros, load_sem, sem):
    size = out.shape[2] // groups
    span = groups + 1
    loads = []
    for pair in range(groups // 2):
        part = pl.ds(pair * span, span)
        loads.append(pltpu.make_async_copy(packed.at[part], held.at[part], load_sem.at[pair]))
        loads[-1].start()
    zeros[...] = jnp.zeros_like(zeros)

    def move(source, group, column):
        target = out.at[:, :, pl.ds(group * size, size), pl.ds(column * LANES, LANES)]
        return pltpu.make_async_copy(source, target, sem.at[group, column])

    copies = [move(zeros, group, column) for group in range(groups) for column in range(group)]
    for copy in copies:
        copy.start()
    for pair in range(groups // 2):
        loads[pair].wait()
        far = groups - 1 - pair
        moves = [move(held.at[pair * span + column - pair], pair, column) for column in range(pair, groups)]
        moves += [move(held.at[pair * span + column + 1], far, column) for column in range(far, groups)]
        for copy in moves:
            copy.start()
        copies += moves
    for copy in copies:
        copy.wait()


def kernel_body(forcing, coupling, helmholtz, vertical):
    owners = lax.axis_size("ma")
    levels, parts, rows, width = forcing.shape
    size = LANES // owners
    groups = rows // size
    units = groups * (groups + 1) // 2
    stages = 2 + owners.bit_length() - 1
    total = vertical.shape[0]
    block = (levels, parts, size, LANES)
    kinds = coupling.shape[0]
    f32 = jnp.float32
    slab = jax.ShapeDtypeStruct((units,) + block, f32)
    hbm = pl.BlockSpec(memory_space=pl.ANY)
    vmem = pl.BlockSpec(memory_space=pltpu.VMEM)
    results = pl.pallas_call(
        functools.partial(kernel, owners, groups),
        out_shape=[slab, jax.ShapeDtypeStruct((2, SUBLANES, LANES), f32)]
        + [slab] * 6
        + [jax.ShapeDtypeStruct((units, kinds, size, LANES), f32)],
        in_specs=[hbm, hbm, vmem, vmem],
        out_specs=[hbm, vmem] + [hbm] * 7,
        scratch_shapes=[
            pltpu.VMEM((groups, total, 1, LANES), f32),
            pltpu.VMEM((2 * levels * SUBLANES, total * SUBLANES), jnp.bfloat16),
            pltpu.VMEM((LAG + 1, levels, parts, size + 2 * SUBLANES, LANES), f32),
            pltpu.VMEM(block, f32),
            pltpu.VMEM(block, f32),
            pltpu.VMEM((3,) + block, f32),
            pltpu.VMEM(block, f32),
            pltpu.VMEM((LAG + 1,) + block, f32),
            pltpu.VMEM((2, kinds, size, LANES), f32),
            pltpu.VMEM((SEND_SLOTS,) + block, f32),
            pltpu.VMEM((2,) + block, f32),
            pltpu.VMEM((2, total * SUBLANES, parts * LANES), jnp.bfloat16),
            pltpu.VMEM((stages, 2, SUBLANES, LANES), f32),
            pltpu.VMEM((stages, 2, SUBLANES, LANES), f32),
            pltpu.SemaphoreType.DMA((10, units)),
            pltpu.SemaphoreType.DMA((10, units)),
            pltpu.SemaphoreType.DMA((7,)),
            pltpu.SemaphoreType.DMA((4,)),
            pltpu.SemaphoreType.DMA((2,)),
            pltpu.SemaphoreType.DMA((stages,)),
            pltpu.SemaphoreType.DMA((stages,)),
        ],
        compiler_params=pltpu.CompilerParams(collective_id=0, has_side_effects=True, vmem_limit_bytes=60 * 2**20),
        name="richardson",
    )(forcing, coupling, helmholtz.reshape(groups, 1, LANES), vertical)
    solution = pl.pallas_call(
        functools.partial(spread_kernel, groups),
        out_shape=jax.ShapeDtypeStruct(forcing.shape, f32),
        in_specs=[hbm],
        out_specs=hbm,
        scratch_shapes=[
            pltpu.VMEM((units,) + block, f32),
            pltpu.VMEM(block, f32),
            pltpu.SemaphoreType.DMA((groups // 2,)),
            pltpu.SemaphoreType.DMA((groups, groups)),
        ],
        compiler_params=pltpu.CompilerParams(vmem_limit_bytes=60 * 2**20),
        name="spread",
    )(results[0])
    norms = jnp.sqrt(jnp.sum(results[1], axis=(1, 2)) / (total * width * (width + 1)))
    return (solution, norms)


def fits_kernel(forcing, coupling):
    owners, levs = lax.axis_size("ma"), lax.axis_size("lev")
    rows, width = forcing.shape[2:]
    whole = LANES % owners == 0 and (LANES // owners) % SUBLANES == 0
    return whole and levs == 4 and owners >= 4 and width == rows * owners and width % (2 * LANES) == 0 and coupling.shape[0] == 4


def device_body(forcing, coupling, helmholtz, vertical):
    run = kernel_body if fits_kernel(forcing, coupling) else body
    return run(forcing, coupling, helmholtz, vertical)


def solution(mesh):
    in_specs = (P("lev", None, "ma", None), P(None, "ma", None), P(), P())
    out_specs = (P("lev", None, "ma", None), P())
    return jax.shard_map(device_body, mesh=mesh, in_specs=in_specs, out_specs=out_specs, check_vma=False)
```

```python
import functools

import jax
import jax.numpy as jnp
from jax import lax
from jax.experimental import pallas as pl
from jax.experimental.pallas import tpu as pltpu
from jax.sharding import PartitionSpec as P

OFFSETS = (-2, -1, 1, 2)
COLUMN_STEP = 256


def shifted(block, axis, distance):
    devices = range(lax.axis_size(axis))
    route = [(i - distance, i) for i in devices if i - distance in devices]
    return lax.ppermute(block, axis, route)


def swapped(block, axis):
    return lax.ppermute(block, axis, [(i, i ^ 1) for i in range(lax.axis_size(axis))])


def owned_waves(rows, owners, index):
    fold = jnp.arange(rows, dtype=jnp.int32)
    return fold * owners + jnp.where(fold % 2 == 0, index, owners - 1 - index)


def coupling_weights(coupling, rows, owners, target, holder):
    fold = jnp.arange(rows, dtype=jnp.int32)
    waves = owned_waves(rows, owners, target)
    totals = [0.0] * 5
    for place, offset in enumerate(OFFSETS):
        wave = waves + offset
        valid = (wave >= 0) & (wave < rows * owners)
        wave = jnp.clip(wave, 0, rows * owners - 1)
        source_fold = wave // owners
        position = wave % owners
        owner = jnp.where(source_fold % 2 == 0, position, owners - 1 - position)
        delta = source_fold - fold
        own = valid & (owner == holder)
        level = valid & (delta == 0)
        picks = (
            own & (delta == -1),
            own & (delta == 0),
            own & (delta == 1),
            level & (owner == holder - 2),
            level & (owner == holder + 2),
        )
        for kind, pick in enumerate(picks):
            totals[kind] = totals[kind] + coupling[place] * pick.astype(jnp.float32)[:, None]
    return totals


def body(forcing, coupling, helmholtz, vertical):
    owners = lax.axis_size("ma")
    index = lax.axis_index("ma")
    partner = index + 1 - 2 * (index % 2)
    levels, _, rows, width = forcing.shape
    all_levels = levels * lax.axis_size("lev")
    start = lax.axis_index("lev") * levels
    weights = lax.dynamic_slice_in_dim(vertical, start, levels, 0)
    diagonal = lax.dynamic_slice_in_dim(jnp.diagonal(vertical), start, levels, 0)
    waves = owned_waves(rows, owners, index)
    positions = jnp.arange(width, dtype=jnp.int32)
    live = (positions[None, :] >= waves[:, None]).astype(jnp.float32)
    scale = 1.0 / (1.0 + helmholtz[None, :] * diagonal[:, None])

    mine = coupling_weights(coupling, rows, owners, index, index)
    theirs = coupling_weights(swapped(coupling, "ma"), rows, owners, partner, index)
    mine = lax.optimization_barrier(jnp.stack(mine))
    theirs = lax.optimization_barrier(jnp.stack(theirs))

    groups = max(width // COLUMN_STEP, 1)
    if width % COLUMN_STEP or rows % groups:
        groups = 1
    size = rows // groups
    solution = jnp.zeros_like(forcing)
    first_sum = jnp.float32(0)
    second_sum = jnp.float32(0)
    sent = []
    for group in range(groups):
        low, left = group * size, group * size * owners
        rhs = forcing[:, :, low : low + size, left:] * live[low : low + size, left:]
        first = lax.optimization_barrier(scale[:, None, None, left:] * rhs)
        below = shifted(first, "ma", 2)
        above = shifted(first, "ma", -2)
        gathered = lax.all_gather(first, "lev", axis=0, tiled=True)
        sent.append((first, below, above, gathered))
    for group in range(groups):
        low, left = group * size, group * size * owners
        first, below, above, gathered = sent[group]
        mask = live[low : low + size, left:]
        rhs = forcing[:, :, low : low + size, left:] * mask
        column_scale = scale[:, None, None, left:]
        empty = jnp.zeros_like(first[:, :, :1])
        before, after = empty, empty
        if group > 0:
            before = sent[group - 1][0][:, :, -1:, size * owners :]
        if group < groups - 1:
            gap = ((0, 0), (0, 0), (0, 0), (size * owners, 0))
            after = jnp.pad(sent[group + 1][0][:, :, :1], gap)
        down = jnp.concatenate([before, first[:, :, :-1]], axis=2)
        up = jnp.concatenate([first[:, :, 1:], after], axis=2)
        fields = (down, first, up, below, above)

        def combined(table):
            part = table[:, low : low + size, left:]
            return sum(part[kind][None, None] * field for kind, field in enumerate(fields))

        received = swapped(combined(theirs), "ma")
        mixed = jnp.einsum("kl,lcin->kcin", weights, gathered, precision=lax.Precision.HIGH)
        result = first + helmholtz[None, None, None, left:] * mixed
        result = result + combined(mine) + received
        residual = rhs - result * mask
        first_sum = first_sum + jnp.sum(rhs * rhs)
        second_sum = second_sum + jnp.sum(residual * residual)
        update = first + column_scale * residual
        solution = lax.dynamic_update_slice(solution, update, (0, 0, low, left))
    sums = lax.psum(jnp.stack([first_sum, second_sum]), ("ma", "lev"))
    norms = jnp.sqrt(sums / (all_levels * width * (width + 1)))
    return (solution, norms)


LANES = 128
SUBLANES = 8
AHEAD = 6
WEIGHT_AHEAD = 20
WHOLE = 10
RELAY_AHEAD = 12
JOIN_AHEAD = 2
LAG = 3
SEND_SLOTS = 4
MESH = pl.DeviceIdType.MESH


def unit_place(unit, groups):
    pair, step = unit // (groups + 1), unit % (groups + 1)
    far = (step + pair) // groups
    group = pair + far * (groups - 1 - 2 * pair)
    column = (pair + step) * (1 - far) + (step - 1) * far
    return group, column


def tile_weights(coupling, fold, column, owners, target, holder):
    even = (fold & 1) == 0
    place = jnp.where(even, target, owners - 1 - target)
    wave = fold * owners + place
    totals = [jnp.zeros(fold.shape, jnp.float32)] * 5
    for kind, offset in enumerate(OFFSETS):
        moved = place + offset
        delta = jnp.where(moved < 0, -1, jnp.where(moved >= owners, 1, 0))
        position = moved - delta * owners
        parity = (fold + delta) & 1
        owner = jnp.where(parity == 0, position, owners - 1 - position)
        live = (wave + offset >= 0) & (column >= wave + offset)
        value = jnp.where(live, coupling[kind], 0.0)
        where_own = jnp.where(owner == holder, delta, 9)
        where_level = jnp.where(delta == 0, owner - holder, 9)
        picks = (where_own == -1, where_own == 0, where_own == 1, where_level == -2, where_level == 2)
        for i, pick in enumerate(picks):
            totals[i] = totals[i] + jnp.where(pick, value, 0.0)
    return totals


def prepare(vertical, helmholtz, mixing, scale, blocks, levels):
    total = vertical.shape[0]
    depth, full = levels * SUBLANES, total * SUBLANES
    bits = SUBLANES.bit_length() - 1

    def iota(shape, axis):
        return lax.broadcasted_iota(jnp.int32, shape, axis)

    def one_hot(pick):
        return jnp.where(pick, 1.0, 0.0).astype(jnp.bfloat16)

    values = vertical[...]
    coarse = values.astype(jnp.bfloat16)
    fine = (values - coarse.astype(jnp.float32)).astype(jnp.bfloat16)
    pick = one_hot((iota((depth, total), 0) >> bits) + blocks[0] * levels == iota((depth, total), 1))
    level = iota((total, full), 1) >> bits
    source = level + blocks[0] * levels
    for i, block in enumerate(blocks):
        source = jnp.where(level >= i * levels, level + (block - i) * levels, source)
    spread = one_hot(source == iota((total, full), 0))
    same = (iota((depth, full), 0) & (SUBLANES - 1)) == (iota((depth, full), 1) & (SUBLANES - 1))
    for i, part in enumerate((coarse, fine)):
        chosen = jnp.dot(pick, part, preferred_element_type=jnp.float32).astype(jnp.bfloat16)
        wide = jnp.dot(chosen, spread, preferred_element_type=jnp.float32)
        mixing[pl.ds(i * depth, depth)] = jnp.where(same, wide, 0.0).astype(jnp.bfloat16)
    here = iota((total, total), 0) == iota((total, total), 1)
    diagonal = jnp.sum(jnp.where(here, values, 0.0), axis=1, keepdims=True)
    diagonal = jnp.broadcast_to(diagonal, (total, LANES))[:, None, :]
    for column in range(scale.shape[0]):
        scale[column] = 1.0 / (1.0 + helmholtz[column][None] * diagonal)


def joined_sums(source, slots, send, recv, base, place, devices):
    count = len(devices) + 1

    def exchange(shift, slot):
        return pltpu.make_async_remote_copy(
            src_ref=source,
            dst_ref=slots.at[slot],
            send_sem=send.at[base + shift - 1],
            recv_sem=recv.at[base + shift - 1],
            device_id=devices[shift - 1],
            device_id_type=MESH,
        )

    for shift in range(1, count):
        exchange(shift, place).start()
    slots[place] = source[...]
    for shift in range(1, count):
        exchange(shift, place).wait_send()
        exchange(shift, (place + count - shift) % count).wait_recv()
    return sum(slots[slot] for slot in range(count))


def kernel(
    owners,
    groups,
    forcing,
    coupling,
    helmholtz,
    vertical,
    out,
    sums,
    below_in,
    above_in,
    far_in,
    twin_in,
    far_twin_in,
    cross_in,
    weight_in,
    scale,
    mixing,
    ext,
    low,
    high,
    remote,
    cross,
    mine,
    weights,
    partial,
    result,
    matrix,
    total_out,
    level_in,
    owner_in,
    send,
    recv,
    load_sem,
    remote_sem,
    store_sem,
    sum_send,
    sum_recv,
):
    levels = forcing.shape[0]
    size = below_in.shape[3]
    units = below_in.shape[0]
    rows = groups * size
    index = lax.axis_index("ma")
    lev = lax.axis_index("lev")
    has_low = index >= 2
    has_high = index < owners - 2
    to_low = {"ma": jnp.maximum(index - 2, 0), "lev": lev}
    to_high = {"ma": jnp.minimum(index + 2, owners - 1), "lev": lev}
    partner = index + 1 - 2 * (index % 2)
    to_cross = {"ma": partner, "lev": lev}
    twin = lev + 1 - 2 * (lev % 2)
    far = (lev + 2) % 4
    far_twin = (twin + 2) % 4
    to_twin = {"ma": index, "lev": twin}
    to_far = {"ma": index, "lev": far}
    share = coupling.shape[0] // 4
    others = [{"ma": (index + shift) % owners, "lev": lev} for shift in range(1, owners)]
    mates = [{"ma": index, "lev": (lev + shift) % 4} for shift in range(1, 4)]

    def cut(group, column):
        return pl.ds(pl.multiple_of(group * size, size), size), pl.ds(pl.multiple_of(column * LANES, LANES), LANES)

    def remote_copy(kind, unit, source, target, device):
        return pltpu.make_async_remote_copy(
            src_ref=source,
            dst_ref=target,
            send_sem=send.at[kind, unit],
            recv_sem=recv.at[kind, unit],
            device_id=device,
            device_id_type=MESH,
        )

    def tile(unit):
        group, column = unit_place(unit, groups)
        r, c = cut(group, column)
        return forcing.at[:, :, r, c]

    def copy_high(unit):
        return remote_copy(0, unit, tile(unit), below_in.at[unit], to_high)

    def copy_low(unit):
        return remote_copy(1, unit, tile(unit), above_in.at[unit], to_low)

    def copy_far(unit):
        return remote_copy(2, unit, tile(unit), far_in.at[unit], to_far)

    def copy_twin(unit):
        return remote_copy(3, unit, tile(unit), twin_in.at[unit], to_twin)

    def copy_far_twin(unit):
        return remote_copy(4, unit, far_in.at[unit], far_twin_in.at[unit], to_twin)

    def copy_cross(unit):
        return remote_copy(5, unit, partial.at[unit % SEND_SLOTS], cross_in.at[unit], to_cross)

    def held(unit, owner):
        return weight_in.at[unit, pl.ds(owner * share, share)]

    def copy_weight(unit):
        group, column = unit_place(unit, groups)
        r, c = cut(group, column)
        source = coupling.at[pl.ds(lev * share, share), r, c]
        return remote_copy(6, unit, source, held(unit, lev), to_cross)

    def copy_weights(unit):
        group, column = unit_place(unit, groups)
        r, c = cut(group, column)
        return remote_copy(6, unit, coupling.at[:, r, c], weight_in.at[unit], to_cross)

    def relay_twin(unit):
        return remote_copy(7, unit, held(unit, lev), held(unit, lev), to_twin)

    def relay_far(unit):
        return remote_copy(8, unit, held(unit, lev), held(unit, lev), to_far)

    def relay_far_twin(unit):
        return remote_copy(9, unit, held(unit, far), held(unit, far), to_twin)

    def from_twin(unit):
        return remote_copy(7, unit, held(unit, twin), held(unit, twin), to_twin)

    def from_far(unit):
        return remote_copy(8, unit, held(unit, far), held(unit, far), to_far)

    def from_far_twin(unit):
        return remote_copy(9, unit, held(unit, far_twin), held(unit, far_twin), to_twin)

    def start_sends(unit):
        @pl.when(has_high)
        def _():
            copy_high(unit).start()

        @pl.when(has_low)
        def _():
            copy_low(unit).start()

        copy_far(unit).start()
        copy_twin(unit).start()

    def near_loads(unit):
        group, column = unit_place(unit, groups)
        r, c = cut(group, column)
        slot = unit % (LAG + 1)
        first = group * size
        ahead = pl.ds(pl.multiple_of(jnp.maximum(first - SUBLANES, 0), SUBLANES), SUBLANES)
        behind = pl.ds(pl.multiple_of(jnp.minimum(first + size, rows - SUBLANES), SUBLANES), SUBLANES)
        return [
            pltpu.make_async_copy(forcing.at[:, :, ahead, c], ext.at[slot, :, :, pl.ds(0, SUBLANES)], load_sem.at[0]),
            pltpu.make_async_copy(forcing.at[:, :, r, c], ext.at[slot, :, :, pl.ds(SUBLANES, size)], load_sem.at[1]),
            pltpu.make_async_copy(forcing.at[:, :, behind, c], ext.at[slot, :, :, pl.ds(SUBLANES + size, SUBLANES)], load_sem.at[2]),
            pltpu.make_async_copy(coupling.at[:, r, c], weights.at[0], load_sem.at[3]),
        ]

    def low_load(unit):
        return pltpu.make_async_copy(below_in.at[unit], low, load_sem.at[4])

    def high_load(unit):
        return pltpu.make_async_copy(above_in.at[unit], high, load_sem.at[5])

    def weight_load(unit):
        return pltpu.make_async_copy(weight_in.at[unit], weights.at[1], load_sem.at[6])

    def remote_loads(unit):
        return [
            pltpu.make_async_copy(twin_in.at[unit], remote.at[0], remote_sem.at[0]),
            pltpu.make_async_copy(far_in.at[unit], remote.at[1], remote_sem.at[1]),
            pltpu.make_async_copy(far_twin_in.at[unit], remote.at[2], remote_sem.at[2]),
            pltpu.make_async_copy(cross_in.at[unit], cross, remote_sem.at[3]),
        ]

    def store(unit):
        return pltpu.make_async_copy(result.at[unit % 2], out.at[unit], store_sem.at[unit % 2])

    def near_step(unit):
        group, column = unit_place(unit, groups)
        slot = unit % (LAG + 1)
        fold = group * size + lax.broadcasted_iota(jnp.int32, (size, LANES), 0)
        lane = column * LANES + lax.broadcasted_iota(jnp.int32, (size, LANES), 1)
        own = tile_weights(weights[0], fold, lane, owners, index, index)
        theirs = tile_weights(weights[1], fold, lane, owners, partner, index)
        for c in range(2):
            fields = (
                ext[slot, :, c, SUBLANES - 1 : SUBLANES - 1 + size, :],
                ext[slot, :, c, SUBLANES : SUBLANES + size, :],
                ext[slot, :, c, SUBLANES + 1 : SUBLANES + 1 + size, :],
                low[:, c],
                high[:, c],
            )
            mine[slot, :, c] = sum(w[None] * f for w, f in zip(own, fields))
            partial[unit % SEND_SLOTS, :, c] = sum(w[None] * f for w, f in zip(theirs, fields))

    def final_step(unit):
        group, column = unit_place(unit, groups)
        slot = unit % (LAG + 1)
        own_scale = scale[column, pl.ds(lev * levels, levels)]
        helm = helmholtz[column][None]
        for tall in range(size // SUBLANES):
            start = tall * SUBLANES
            for c in range(2):
                lanes = pl.ds(c * LANES, LANES)
                for source, block in enumerate((lev, twin, far, far_twin)):
                    if source == 0:
                        raw = ext[slot, :, c, SUBLANES + start : 2 * SUBLANES + start, :]
                    else:
                        raw = remote[source - 1, :, c, start : start + SUBLANES, :]
                    value = raw * scale[column, pl.ds(block * levels, levels)]
                    value = value.reshape(levels * SUBLANES, LANES)
                    coarse = value.astype(jnp.bfloat16)
                    fine = (value - coarse.astype(jnp.float32)).astype(jnp.bfloat16)
                    depth = levels * SUBLANES
                    rows_of = pl.ds(source * depth, depth)
                    matrix[0, rows_of, lanes] = coarse
                    matrix[1, rows_of, lanes] = fine
            both = jnp.dot(mixing[...], matrix[0], preferred_element_type=jnp.float32)
            rest = jnp.dot(mixing[:depth], matrix[1], preferred_element_type=jnp.float32)
            total = both[:depth] + both[depth:] + rest
            fold = group * size + start + lax.broadcasted_iota(jnp.int32, (SUBLANES, LANES), 0)
            lane = column * LANES + lax.broadcasted_iota(jnp.int32, (SUBLANES, LANES), 1)
            place = jnp.where((fold & 1) == 0, index, owners - 1 - index)
            mask = (lane >= fold * owners + place).astype(jnp.float32)[None]
            for c in range(2):
                mixed = total[:, c * LANES : (c + 1) * LANES].reshape(levels, SUBLANES, LANES)
                rhs = ext[slot, :, c, SUBLANES + start : 2 * SUBLANES + start, :] * mask
                first = own_scale * rhs
                near = mine[slot, :, c, start : start + SUBLANES, :] + cross[:, c, start : start + SUBLANES, :]
                applied = first + helm * mixed + own_scale * near
                residual = rhs - applied * mask
                result[unit % 2, :, c, start : start + SUBLANES, :] = first + own_scale * residual
                sums[0] += jnp.sum(rhs * rhs, axis=0)
                sums[1] += jnp.sum(residual * residual, axis=0)

    barrier = pltpu.get_barrier_semaphore()
    for device in others + mates:
        pl.semaphore_signal(barrier, inc=1, device_id=device, device_id_type=MESH)
    pl.semaphore_wait(barrier, len(others) + len(mates))

    def begin(unit, carry):
        start_sends(unit)
        return carry

    def begin_weights(unit, carry):
        copy_weights(unit).start()
        return carry

    def begin_weight(unit, carry):
        copy_weight(unit).start()
        return carry

    whole = min(WHOLE, units)
    lax.fori_loop(0, min(AHEAD, units), begin, 0)
    lax.fori_loop(0, whole, begin_weights, 0)
    lax.fori_loop(whole, min(WEIGHT_AHEAD, units), begin_weight, 0)
    sums[...] = jnp.zeros_like(sums)
    prepare(vertical, helmholtz, mixing, scale, (lev, twin, far, far_twin), levels)

    def relay(unit, carry):
        copy_weight(unit).wait()
        relay_twin(unit).start()
        relay_far(unit).start()
        return carry

    lax.fori_loop(whole, min(RELAY_AHEAD, units), relay, 0)

    def step(now, carry):
        @pl.when(now + AHEAD < units)
        def _():
            start_sends(now + AHEAD)

        @pl.when(now + WEIGHT_AHEAD < units)
        def _():
            copy_weight(now + WEIGHT_AHEAD).start()

        @pl.when(now < units)
        def _():
            for copy in near_loads(now):
                copy.start()

        @pl.when(now + RELAY_AHEAD < units)
        def _():
            relay(now + RELAY_AHEAD, 0)

        @pl.when((now + JOIN_AHEAD >= whole) & (now + JOIN_AHEAD < units))
        def _():
            unit = now + JOIN_AHEAD
            from_far(unit).wait_recv()
            relay_far_twin(unit).start()

        @pl.when(now < whole)
        def _():
            copy_weights(now).wait()

        @pl.when((now >= whole) & (now < units))
        def _():
            from_twin(now).wait_recv()
            from_far_twin(now).wait_recv()

        @pl.when(now < units)
        def _():
            weight_load(now).start()

            @pl.when(has_low)
            def _():
                copy_high(now).wait_recv()
                low_load(now).start()

            @pl.when(jnp.logical_not(has_low))
            def _():
                pltpu.make_async_copy(tile(now), low, load_sem.at[4]).start()

            @pl.when(has_high)
            def _():
                copy_low(now).wait_recv()
                high_load(now).start()

            @pl.when(jnp.logical_not(has_high))
            def _():
                pltpu.make_async_copy(tile(now), high, load_sem.at[5]).start()

        @pl.when(now >= LAG)
        def _():
            unit = now - LAG
            for copy in remote_loads(unit):
                copy.wait()

            @pl.when(unit >= 2)
            def _():
                store(unit - 2).wait()

            final_step(unit)
            store(unit).start()

        @pl.when(now < units)
        def _():
            for copy in near_loads(now):
                copy.wait()
            low_load(now).wait()
            high_load(now).wait()
            weight_load(now).wait()

            @pl.when(now >= SEND_SLOTS)
            def _():
                copy_cross(now - SEND_SLOTS).wait_send()

            near_step(now)
            copy_cross(now).start()
            copy_far(now).wait()
            copy_far_twin(now).start()

            @pl.when(has_high)
            def _():
                copy_high(now).wait_send()

            @pl.when(has_low)
            def _():
                copy_low(now).wait_send()


        @pl.when((now >= whole) & (now < units))
        def _():
            relay_twin(now).wait_send()
            relay_far(now).wait_send()
            relay_far_twin(now).wait_send()

        @pl.when((now >= LAG - 1) & (now < units + LAG - 1))
        def _():
            unit = now - (LAG - 1)
            copy_twin(unit).wait()
            copy_far_twin(unit).wait()
            copy_cross(unit).wait_recv()
            for copy in remote_loads(unit):
                copy.start()

        return carry

    lax.fori_loop(0, units + LAG, step, 0)
    for unit in range(max(units - SEND_SLOTS, 0), units):
        copy_cross(unit).wait_send()
    total_out[0] = sums[...]
    total_out[1] = joined_sums(total_out.at[0], level_in, sum_send, sum_recv, 0, lev, mates)
    sums[...] = joined_sums(total_out.at[1], owner_in, sum_send, sum_recv, len(mates), index, others)
    for unit in range(max(units - 2, 0), units):
        store(unit).wait()


def spread_kernel(groups, packed, out, held, zeros, load_sem, sem):
    size = out.shape[2] // groups
    span = groups + 1
    loads = []
    for pair in range(groups // 2):
        part = pl.ds(pair * span, span)
        loads.append(pltpu.make_async_copy(packed.at[part], held.at[part], load_sem.at[pair]))
        loads[-1].start()
    zeros[...] = jnp.zeros_like(zeros)

    def move(source, group, column):
        target = out.at[:, :, pl.ds(group * size, size), pl.ds(column * LANES, LANES)]
        return pltpu.make_async_copy(source, target, sem.at[group, column])

    copies = [move(zeros, group, column) for group in range(groups) for column in range(group)]
    for copy in copies:
        copy.start()
    for pair in range(groups // 2):
        loads[pair].wait()
        far = groups - 1 - pair
        moves = [move(held.at[pair * span + column - pair], pair, column) for column in range(pair, groups)]
        moves += [move(held.at[pair * span + column + 1], far, column) for column in range(far, groups)]
        for copy in moves:
            copy.start()
        copies += moves
    for copy in copies:
        copy.wait()


def kernel_body(forcing, coupling, helmholtz, vertical):
    owners = lax.axis_size("ma")
    levels, parts, rows, width = forcing.shape
    size = LANES // owners
    groups = rows // size
    units = groups * (groups + 1) // 2
    total = vertical.shape[0]
    block = (levels, parts, size, LANES)
    kinds = coupling.shape[0]
    f32 = jnp.float32
    slab = jax.ShapeDtypeStruct((units,) + block, f32)
    hbm = pl.BlockSpec(memory_space=pl.ANY)
    vmem = pl.BlockSpec(memory_space=pltpu.VMEM)
    results = pl.pallas_call(
        functools.partial(kernel, owners, groups),
        out_shape=[slab, jax.ShapeDtypeStruct((2, SUBLANES, LANES), f32)]
        + [slab] * 6
        + [jax.ShapeDtypeStruct((units, kinds, size, LANES), f32)],
        in_specs=[hbm, hbm, vmem, vmem],
        out_specs=[hbm, vmem] + [hbm] * 7,
        scratch_shapes=[
            pltpu.VMEM((groups, total, 1, LANES), f32),
            pltpu.VMEM((2 * levels * SUBLANES, total * SUBLANES), jnp.bfloat16),
            pltpu.VMEM((LAG + 1, levels, parts, size + 2 * SUBLANES, LANES), f32),
            pltpu.VMEM(block, f32),
            pltpu.VMEM(block, f32),
            pltpu.VMEM((3,) + block, f32),
            pltpu.VMEM(block, f32),
            pltpu.VMEM((LAG + 1,) + block, f32),
            pltpu.VMEM((2, kinds, size, LANES), f32),
            pltpu.VMEM((SEND_SLOTS,) + block, f32),
            pltpu.VMEM((2,) + block, f32),
            pltpu.VMEM((2, total * SUBLANES, parts * LANES), jnp.bfloat16),
            pltpu.VMEM((2, 2, SUBLANES, LANES), f32),
            pltpu.VMEM((4, 2, SUBLANES, LANES), f32),
            pltpu.VMEM((owners, 2, SUBLANES, LANES), f32),
            pltpu.SemaphoreType.DMA((10, units)),
            pltpu.SemaphoreType.DMA((10, units)),
            pltpu.SemaphoreType.DMA((7,)),
            pltpu.SemaphoreType.DMA((4,)),
            pltpu.SemaphoreType.DMA((2,)),
            pltpu.SemaphoreType.DMA((owners + 2,)),
            pltpu.SemaphoreType.DMA((owners + 2,)),
        ],
        compiler_params=pltpu.CompilerParams(collective_id=0, has_side_effects=True, vmem_limit_bytes=60 * 2**20),
        name="richardson",
    )(forcing, coupling, helmholtz.reshape(groups, 1, LANES), vertical)
    solution = pl.pallas_call(
        functools.partial(spread_kernel, groups),
        out_shape=jax.ShapeDtypeStruct(forcing.shape, f32),
        in_specs=[hbm],
        out_specs=hbm,
        scratch_shapes=[
            pltpu.VMEM((units,) + block, f32),
            pltpu.VMEM(block, f32),
            pltpu.SemaphoreType.DMA((groups // 2,)),
            pltpu.SemaphoreType.DMA((groups, groups)),
        ],
        compiler_params=pltpu.CompilerParams(vmem_limit_bytes=60 * 2**20),
        name="spread",
    )(results[0])
    norms = jnp.sqrt(jnp.sum(results[1], axis=(1, 2)) / (total * width * (width + 1)))
    return (solution, norms)


def fits_kernel(forcing, coupling):
    owners, levs = lax.axis_size("ma"), lax.axis_size("lev")
    rows, width = forcing.shape[2:]
    whole = LANES % owners == 0 and (LANES // owners) % SUBLANES == 0
    return whole and levs == 4 and owners >= 4 and width == rows * owners and width % (2 * LANES) == 0 and coupling.shape[0] == 4


def device_body(forcing, coupling, helmholtz, vertical):
    run = kernel_body if fits_kernel(forcing, coupling) else body
    return run(forcing, coupling, helmholtz, vertical)


def solution(mesh):
    in_specs = (P("lev", None, "ma", None), P(None, "ma", None), P(), P())
    out_specs = (P("lev", None, "ma", None), P())
    return jax.shard_map(device_body, mesh=mesh, in_specs=in_specs, out_specs=out_specs, check_vma=False)
```
